256 devices in a mesh: graph: 64 (over z, y, core), feat: 4 (over x).
Axes of the slice: x: 4, y: 4, z: 8, core: 2. Of those that a mesh axis runs over, the one named last changes fastest.
Arguments:
- node_feats: bfloat16 [20480, 512], P(('graph', 'feat')), may hold values from -6 to 6
- edge_feats: bfloat16 [131072, 512], P(('graph', 'feat')), may hold values from -6 to 6
- senders: int32 [131072], P(('graph', 'feat')), may hold values from 0 to 319
- receiver_ref: int32 [131072], P(('graph', 'feat')), may hold values from 0 to 6463, as said below
- send_list: int32 [64, 64, 96], P('graph'), may hold values from 0 to 319, as said below
- edge_count: int32 [64], P('graph'), may hold values from 1024 to 2048, as said below
- edge_w1: bfloat16 [1536, 512], replicated, may hold values from -0.15625 to 0.15625
- edge_w2: bfloat16 [512, 512], replicated, may hold values from -0.25 to 0.25
- edge_gain: bfloat16 [512], replicated, may hold values from 0.099609375 to 1.8984375
- edge_shift: bfloat16 [512], replicated, may hold values from -3 to 3
- node_w1: bfloat16 [1024, 512], replicated, may hold values from -0.1875 to 0.1875
- node_w2: bfloat16 [512, 512], replicated, may hold values from -0.25 to 0.25
- node_gain: bfloat16 [512], replicated, may hold values from 0.099609375 to 1.8984375
- node_shift: bfloat16 [512], replicated, may hold values from -3 to 3
Outputs:
- new_edges: bfloat16 [131072, 512], P(('graph', 'feat'))
- new_nodes: bfloat16 [20480, 512], P(('graph', 'feat'))
The draws below stay inside these ranges and needn't reach their ends.
Inputs may be any that keep to these rules, and one draw needn't show every extreme that they name: `senders`: local node indices of the edge's own region. `receiver_ref`: A value below 320 is a node of the edge's own region. Otherwise q = value - 320 names slot q % 96 of the list that region s = q // 96 keeps for the edge's region; s is never the edge's own region, and when s is more than 2 steps away around the region order (either direction, wrapping) the slot is below 16. In every draw each region has an edge on slot 95 of the next region and an edge on slot 15 of the region 3 steps on. Each list send_list[s, g] holds 96 distinct local node indices of region s. Region g's live edges are its first edge_count[g] edge slots; some region has all 2048 live.
All inputs are finite; a program needn't handle non-finite values.
Results may differ from the reference program's by a relative error of at most 0.009.
Values may be sent and summed in bfloat16 or wider, within the bound.
No kernel may reach another device: no remote copies, remote signals or barrier semaphores. Data moves between devices by JAX's collectives and lax.ppermute only.
A program may use at most 128 MiB of HBM per device.

```python
import jax
import jax.numpy as jnp
from jax import lax

D = 512
HID = 512
NODE_DEV = 320
EDGE_DEV = 2048
SLOT = 96
FAR_SLOT = 16
REACH = 2
NODES = 20480
EDGES = 131072
N_GRAPH = 64


def draw_send_list(key, part):
    random_scores = jax.random.randint(key, (N_GRAPH * N_GRAPH, NODE_DEV), 0, 1 << 16)
    distinct_scores = random_scores * NODE_DEV + jnp.arange(NODE_DEV, dtype=jnp.int32)[None, :]
    ranked = jnp.argsort(distinct_scores, axis=1, stable=True)[:, :SLOT]
    return ranked.reshape(N_GRAPH, N_GRAPH, SLOT).astype(jnp.int32)


def draw_receiver_ref(key, part):
    subkeys = jax.random.split(key, 5)
    total_edges = N_GRAPH * EDGE_DEV
    shard_index = jnp.arange(total_edges, dtype=jnp.int32) // EDGE_DEV
    position = jnp.arange(total_edges, dtype=jnp.int32) % EDGE_DEV
    category = jax.random.randint(subkeys[0], (total_edges,), 0, 10)
    local_node = jax.random.randint(subkeys[1], (total_edges,), 0, NODE_DEV)
    near_pick = jax.random.randint(subkeys[2], (total_edges,), 0, 2 * REACH)
    near_offset = jnp.where(near_pick < REACH, near_pick - REACH, near_pick - REACH + 1)
    far_offset = REACH + 1 + jax.random.randint(subkeys[3], (total_edges,), 0, N_GRAPH - 2 * REACH - 1)
    near_slot = jax.random.randint(subkeys[4], (total_edges,), 0, SLOT)
    far_slot = near_slot % FAR_SLOT
    near_offset = jnp.where(position == 1, 1, near_offset)
    near_slot = jnp.where(position == 1, SLOT - 1, near_slot)
    far_offset = jnp.where(position == 0, REACH + 1, far_offset)
    far_slot = jnp.where(position == 0, FAR_SLOT - 1, far_slot)
    category = jnp.where(position == 0, 0, jnp.where(position == 1, 1, category))
    near_value = NODE_DEV + (shard_index + near_offset) % N_GRAPH * SLOT + near_slot
    far_value = NODE_DEV + (shard_index + far_offset) % N_GRAPH * SLOT + far_slot
    return jnp.where(category == 0, far_value, jnp.where(category < 5, near_value, local_node)).astype(jnp.int32)


def draw_edge_count(key, part):
    count_key, full_key = jax.random.split(key)
    edge_totals = jax.random.randint(count_key, (N_GRAPH,), EDGE_DEV // 2, EDGE_DEV + 1)
    fullest = jax.random.randint(full_key, (), 0, N_GRAPH)
    return jnp.where(jnp.arange(N_GRAPH) == fullest, EDGE_DEV, edge_totals).astype(jnp.int32)


def place_ends(drawn, rng, low, largest):
    index_at = [jax.random.randint(jax.random.fold_in(rng, axis), (), 0, length) for axis, length in enumerate(drawn.shape)]
    main_axis = drawn.shape.index(max(drawn.shape))
    neighbour = index_at[:main_axis] + [(index_at[main_axis] + 1) % drawn.shape[main_axis]] + index_at[main_axis + 1:]
    return drawn.at[tuple(index_at)].set(low).at[tuple(neighbour)].set(largest)


def levels(stream_key, dims, cuts, low, high):
    loudness, own = 1.0, jax.random.fold_in(stream_key, 6)
    for dim, parts in cuts:
        steps = jnp.exp(jax.random.uniform(jax.random.fold_in(own, dim), (parts,), jnp.float32, low / len(cuts), high / len(cuts)))
        loudness = loudness * jnp.repeat(steps, dims[dim] // parts).reshape([-1 if axis == dim else 1 for axis in range(len(dims))])
    return loudness


def centred(stream_key, dims, width, reach, pieces=(), kind=jnp.bfloat16):
    entries = width * jax.random.normal(stream_key, dims, jnp.float32)
    if pieces:
        entries = entries * levels(stream_key, dims, pieces, -0.22, 0.18)
    return jnp.clip(entries, -reach, reach).astype(kind)


def setup_inputs(seed: int = 0) -> dict:
    splits = jax.random.split(jax.random.key(seed), 15)
    node_feats = centred(splits[0], (NODES, D), 1.0, 6.0, ((0, 256),))
    edge_feats = centred(splits[1], (EDGES, D), 1.0, 6.0, ((0, 256),))
    senders = place_ends(jax.random.randint(splits[2], (EDGES,), 0, NODE_DEV), jax.random.fold_in(splits[2], 1), 0, NODE_DEV - 1).astype(jnp.int32)
    receiver_ref = draw_receiver_ref(jax.random.fold_in(splits[14], 71), 0)
    send_list = draw_send_list(jax.random.fold_in(splits[14], 71), 0)
    edge_count = draw_edge_count(jax.random.fold_in(splits[14], 71), 0)
    edge_w1 = centred(splits[6], (3 * D, HID), (3 * D) ** -0.5, 0.15625)
    edge_w2 = centred(splits[7], (HID, D), HID ** -0.5, 0.25)
    edge_gain = jnp.clip(1.0 + 0.18 * jax.random.normal(splits[8], (D,), jnp.float32), 0.099609375, 1.8984375).astype(jnp.bfloat16)
    edge_shift = centred(splits[9], (D,), 0.5, 3.0)
    node_w1 = centred(splits[10], (2 * D, HID), (2 * D) ** -0.5, 0.1875)
    node_w2 = centred(splits[11], (HID, D), HID ** -0.5, 0.25)
    node_gain = jnp.clip(1.0 + 0.18 * jax.random.normal(splits[12], (D,), jnp.float32), 0.099609375, 1.8984375).astype(jnp.bfloat16)
    node_shift = centred(splits[13], (D,), 0.5, 3.0)
    return dict(node_feats=node_feats, edge_feats=edge_feats, senders=senders, receiver_ref=receiver_ref, send_list=send_list, edge_count=edge_count, edge_w1=edge_w1, edge_w2=edge_w2, edge_gain=edge_gain, edge_shift=edge_shift, node_w1=node_w1, node_w2=node_w2, node_gain=node_gain, node_shift=node_shift)


epsilon = 1e-05

def layer_norm(outputs, norm_gain, norm_shift):
    average = lax.optimization_barrier(jnp.mean(outputs, axis=-1, keepdims=True))
    centered = outputs - average
    variance = lax.optimization_barrier(jnp.mean(centered * centered, axis=-1, keepdims=True))
    return centered * lax.rsqrt(variance + epsilon) * norm_gain + norm_shift

def perceptron(inputs, first_weight, second_weight, norm_gain, norm_shift):
    joined = jnp.concatenate(inputs, axis=1)
    activation = jnp.dot(joined, first_weight, preferred_element_type=jnp.float32)
    hidden = jax.nn.silu(activation).astype(jnp.bfloat16)
    outputs = jnp.dot(hidden, second_weight, preferred_element_type=jnp.float32)
    return layer_norm(outputs, norm_gain, norm_shift)

def reference(node_feats, edge_feats, senders, receiver_ref, send_list, edge_count, edge_w1, edge_w2, edge_gain, edge_shift, node_w1, node_w2, node_gain, node_shift):
    positions = jnp.arange(EDGE_DEV, dtype=jnp.int32)

    def shard_step(aggregate, shard_index):
        first_edge = shard_index * EDGE_DEV
        edge_block = lax.dynamic_slice_in_dim(edge_feats, first_edge, EDGE_DEV, 0)
        sender_block = lax.dynamic_slice_in_dim(senders, first_edge, EDGE_DEV, 0)
        ref_block = lax.dynamic_slice_in_dim(receiver_ref, first_edge, EDGE_DEV, 0)
        offset = jnp.maximum(ref_block - NODE_DEV, 0)
        source = offset // SLOT
        slot_index = offset % SLOT
        column = lax.dynamic_index_in_dim(send_list, shard_index, 1, keepdims=False)
        remote = source * NODE_DEV + column[source, slot_index]
        receivers = jnp.where(ref_block < NODE_DEV, shard_index * NODE_DEV + ref_block, remote).astype(jnp.int32)
        sender_rows = node_feats[(shard_index * NODE_DEV + sender_block).astype(jnp.int32)]
        receiver_rows = node_feats[receivers]
        update = edge_block.astype(jnp.float32) + perceptron((edge_block, sender_rows, receiver_rows), edge_w1, edge_w2, edge_gain, edge_shift)
        live_mask = positions < edge_count[shard_index]
        new_rows = jnp.where(live_mask[:, None], update, edge_block.astype(jnp.float32)).astype(jnp.bfloat16)
        messages = jnp.where(live_mask[:, None], new_rows.astype(jnp.float32), 0.0)
        aggregate = aggregate.at[receivers].add(messages)
        return (aggregate, new_rows)
    aggregate, new_edges = lax.scan(shard_step, jnp.zeros((NODES, D), jnp.float32), jnp.arange(N_GRAPH, dtype=jnp.int32))
    new_edges = new_edges.reshape(EDGES, D)
    node_update = node_feats.astype(jnp.float32) + perceptron((node_feats, aggregate.astype(jnp.bfloat16)), node_w1, node_w2, node_gain, node_shift)
    return (new_edges, node_update.astype(jnp.bfloat16))
```

```python
import functools

import jax
import jax.numpy as jnp
from jax import lax
from jax.experimental import pallas as pl
from jax.experimental.pallas import tpu as pltpu
from jax.sharding import PartitionSpec as P

D = 512
Q = 128
FEAT = 4
GROUPS = 64
NODES = 320
OWN = 80
SLOT = 96
FAR = 16
NEAR = SLOT - FAR
EDGES = 512
REGION_EDGES = FEAT * EDGES
OFFSETS = (-2, -1, 1, 2)
FAR_ROWS = GROUPS * FAR
NEAR_ROWS = len(OFFSETS) * NEAR
LIST_ROWS = FAR_ROWS + NEAR_ROWS
EPSILON = 1e-05
F32 = jnp.float32
BF16 = jnp.bfloat16
I32 = jnp.int32


def dot(a, b):
    return jnp.dot(a, b, preferred_element_type=F32)


def iota(shape, dim):
    return lax.broadcasted_iota(I32, shape, dim)


def column(row):
    return jnp.transpose(jnp.broadcast_to(row, (Q, Q)))


def widened(tile, width):
    full, rest = divmod(width, Q)
    parts = [tile] * full + ([tile[:, :rest]] if rest else [])
    return jnp.concatenate(parts, axis=1)


def hot(mask):
    return jnp.where(mask, 1.0, 0.0).astype(BF16)


def call(body, outs, scratch=(), flops=10**8):
    return pl.pallas_call(
        body,
        out_shape=outs,
        scratch_shapes=list(scratch),
        cost_estimate=pl.CostEstimate(flops=flops, bytes_accessed=10**6, transcendentals=0),
    )


def shape(dims, kind):
    return jax.ShapeDtypeStruct(dims, kind)


def project_body(nodes, w1, senders, refs, out, scratch):
    rows = nodes[...]
    sent = dot(rows, w1[D : 2 * D, :]).astype(BF16)
    taken = dot(rows, w1[2 * D : 3 * D, :]).astype(BF16)
    scratch[0:4, :] = senders[...]
    scratch[4:8, :] = refs[...]
    both = scratch[...]
    planes = jnp.concatenate(
        [lax.shift_right_logical(both, 7).astype(F32), (both & 127).astype(F32)], axis=0
    ).astype(BF16)
    for q in range(FEAT):
        cols = slice(q * Q, (q + 1) * Q)
        out[q, 0:OWN, 0:Q] = taken[:, cols]
        out[q, 0:OWN, Q : 2 * Q] = sent[:, cols]
        out[q, OWN : OWN + 16, 0:Q] = planes
        out[q, OWN : OWN + 16, Q : 2 * Q] = jnp.zeros((16, Q), BF16)


def lists_body(lists, select, spread):
    for b in range(8):
        col = column(lists[b : b + 1, :])
        select[b * Q : (b + 1) * Q, :] = hot(widened(col, NODES) == iota((Q, NODES), 1))
    for j in range(4):
        col = column(lists[8 + j : 9 + j, :])[:NEAR]
        at = FAR_ROWS + j * NEAR
        select[at : at + NEAR, :] = hot(widened(col, NODES) == iota((NEAR, NODES), 1))
    for b in range(12):
        spread[:, b * Q : (b + 1) * Q] = hot(
            jnp.broadcast_to(lists[b : b + 1, :], (NODES, Q)) == iota((NODES, Q), 0)
        )


def select_body(table, select, far, near0, near1, near2, near3):
    rows = jnp.concatenate([table[q, 0:OWN, 0:Q] for q in range(FEAT)], axis=0)
    for b in range(4):
        picked = dot(select[b * 256 : (b + 1) * 256, :], rows).astype(BF16)
        far[b * 16 : (b + 1) * 16] = picked.reshape(16, FAR, Q)
    for j, out in enumerate((near0, near1, near2, near3)):
        at = FAR_ROWS + j * NEAR
        out[...] = dot(select[at : at + NEAR, :], rows).astype(BF16)


def local_body(table, rowid, cols, acc):
    region = lax.axis_index("graph")
    both = jnp.concatenate(
        [table[q, 0:OWN, 0:Q] for q in range(FEAT)]
        + [table[q, 0:OWN, Q : 2 * Q] for q in range(FEAT)],
        axis=0,
    )
    for q in range(FEAT):
        planes = table[q, OWN : OWN + 16, 0:Q].astype(F32)
        ids = (planes[0:8] * 128.0 + planes[8:16]).astype(I32)
        ref = ids
        offset = jnp.maximum(ref - NODES, 0)
        source = lax.shift_right_logical(lax.shift_right_logical(offset, 5) * 171, 9)
        slot = offset - source * SLOT
        apart = (source - region) & (GROUPS - 1)
        which = jnp.where(apart >= GROUPS - 2, apart - (GROUPS - 2), apart + 1)
        listed = jnp.where(
            slot < FAR,
            NODES + source * FAR + slot,
            NODES + FAR_ROWS + which * NEAR + slot - FAR,
        )
        ref = jnp.where(ref < NODES, ref, listed)
        rowid[q * 4 : (q + 1) * 4, :] = ref[4:8]
        for r in range(4):
            e = (q * 4 + r) * Q
            taken = column(ref[4 + r : 5 + r, :])
            sent = column(ids[r : r + 1, :])
            cols[e : e + Q, :] = taken
            picks = jnp.concatenate(
                [
                    hot(widened(taken, NODES) == iota((Q, NODES), 1)),
                    hot(widened(sent, NODES) == iota((Q, NODES), 1)),
                ],
                axis=1,
            )
            acc[e : e + Q, :] = dot(picks, both)


def gather_body(acc, cols, far, near0, near1, near2, near3, out):
    table = [far[b * 16 : (b + 1) * 16].reshape(256, Q) for b in range(4)]
    table.append(jnp.concatenate([near0[...], near1[...], near2[...], near3[...]], axis=0))
    for m in range(8):
        col = cols[m * 256 : (m + 1) * 256, :]
        total = acc[m * 256 : (m + 1) * 256, :]
        for b in range(5):
            width = table[b].shape[0]
            picks = hot(widened(col, width) == iota((256, width), 1) + (NODES + b * 256))
            total += dot(picks, table[b])
        at = (m % 2) * 256
        out[m // 2, at : at + 256, :] = total.astype(BF16)


def normed(outputs, gain, shift):
    average = jnp.mean(outputs, axis=-1, keepdims=True)
    centered = outputs - average
    variance = jnp.mean(centered * centered, axis=-1, keepdims=True)
    return centered * lax.rsqrt(variance + EPSILON) * gain + shift


def silu(v):
    return v / (1.0 + jnp.exp(-v))


def edge_body(count, edges, picked, w1, w2, gain, shift, new_edges, messages):
    scale = gain[...].astype(F32)
    move = shift[...].astype(F32)
    first = lax.axis_index("feat") * EDGES
    for m in range(2):
        rows = slice(m * 256, (m + 1) * 256)
        feats = edges[rows, :]
        pre = dot(feats, w1[0:D, :])
        pre += jnp.concatenate([picked[q, rows, :] for q in range(FEAT)], axis=1).astype(F32)
        hidden = silu(pre).astype(BF16)
        update = normed(dot(hidden, w2[...]), scale, move)
        live = first + m * 256 + iota((256, D), 0) < count[0]
        result = feats.astype(F32) + jnp.where(live, update, 0.0)
        new_edges[rows, :] = result.astype(BF16)
        kept = jnp.where(live, result, 0.0).astype(BF16)
        for q in range(FEAT):
            messages[q, rows, :] = kept[:, q * Q : (q + 1) * Q]


def sums_body(messages, rowid, own, far, near0, near1, near2, near3):
    blocks = [(0, 320), (320, 256), (576, 256), (832, 256), (1088, 256), (1344, 320)]
    for base, size in blocks:
        total = jnp.zeros((size, Q), F32)
        for c in range(8):
            q, half = divmod(c, 2)
            ids = jnp.concatenate([rowid[2 * c : 2 * c + 1, :], rowid[2 * c + 1 : 2 * c + 2, :]], axis=1)
            picks = hot(jnp.broadcast_to(ids, (size, 256)) == iota((size, 256), 0) + base)
            total += dot(picks, messages[q, half * 256 : (half + 1) * 256, :])
        if base == 0:
            own[...] = total
        elif base < NODES + FAR_ROWS:
            at = (base - NODES) // FAR
            far[at : at + 16] = total.astype(BF16).reshape(16, FAR, Q)
        else:
            for j, out in enumerate((near0, near1, near2, near3)):
                out[...] = total[j * NEAR : (j + 1) * NEAR].astype(BF16)


def spread_body(spread, own, far, near0, near1, near2, near3, out):
    total = own[...]
    for b in range(4):
        total += dot(
            spread[:, b * 256 : (b + 1) * 256], far[b * 16 : (b + 1) * 16].reshape(256, Q)
        )
    for j, near in enumerate((near0, near1, near2, near3)):
        at = FAR_ROWS + j * Q
        total += dot(spread[:, at : at + NEAR], near[...])
    total = total.astype(BF16)
    for q in range(FEAT):
        out[q] = total[q * OWN : (q + 1) * OWN]


def node_body(nodes, sums, w1, w2, gain, shift, out):
    feats = nodes[...]
    pre = dot(feats, w1[0:D, :])
    pre += dot(jnp.concatenate([sums[q] for q in range(FEAT)], axis=1), w1[D : 2 * D, :])
    hidden = silu(pre).astype(BF16)
    update = normed(dot(hidden, w2[...]), gain[...].astype(F32), shift[...].astype(F32))
    out[...] = (feats.astype(F32) + update).astype(BF16)


def swapped(value, axis):
    return lax.all_to_all(value, axis, split_axis=0, concat_axis=0, tiled=True)


def moved(value, by):
    return lax.ppermute(value, "graph", [(i, (i + by) % GROUPS) for i in range(GROUPS)])


def per_device(
    node_feats,
    edge_feats,
    senders,
    receiver_ref,
    send_list,
    edge_count,
    edge_w1,
    edge_w2,
    edge_gain,
    edge_shift,
    node_w1,
    node_w2,
    node_gain,
    node_shift,
):
    region = lax.axis_index("graph")
    projected = call(
        project_body, shape((FEAT, 96, 256), BF16), [pltpu.VMEM((8, Q), I32)]
    )(node_feats, edge_w1, senders.reshape(4, Q), receiver_ref.reshape(4, Q))
    table = swapped(projected, "feat")

    rows = send_list[0]
    near_lists = [
        jnp.pad(
            lax.dynamic_slice(rows, ((region - d) % GROUPS, FAR), (1, NEAR)),
            ((0, 0), (0, Q - NEAR)),
            constant_values=-1,
        )
        for d in OFFSETS
    ]
    lists = jnp.concatenate([rows[:, :FAR].reshape(8, Q)] + near_lists, axis=0)
    select, spread = call(
        lists_body, (shape((LIST_ROWS, NODES), BF16), shape((NODES, 12 * Q), BF16))
    )(lists)

    near_shape = [shape((NEAR, Q), BF16)] * 4
    far_shape = shape((GROUPS, FAR, Q), BF16)
    far, *near = call(select_body, (far_shape, *near_shape))(table, select)
    far = swapped(far, "graph")
    near = [moved(value, -d) for value, d in zip(near, OFFSETS)]

    rowid, cols, acc = call(
        local_body,
        (
            shape((16, Q), I32),
            shape((REGION_EDGES, Q), I32),
            shape((REGION_EDGES, Q), F32),
        ),
        flops=10**9,
    )(table)
    picked = call(gather_body, shape((FEAT, EDGES, Q), BF16), flops=10**9)(
        acc, cols, far, *near
    )
    picked = swapped(picked, "feat")

    new_edges, messages = pl.pallas_call(
        edge_body,
        out_shape=(shape((EDGES, D), BF16), shape((FEAT, EDGES, Q), BF16)),
        in_specs=[pl.BlockSpec(memory_space=pltpu.SMEM)]
        + [pl.BlockSpec(memory_space=pltpu.VMEM)] * 6,
        cost_estimate=pl.CostEstimate(flops=10**9, bytes_accessed=10**6, transcendentals=0),
    )(
        edge_count,
        edge_feats,
        picked,
        edge_w1,
        edge_w2,
        edge_gain.reshape(1, D),
        edge_shift.reshape(1, D),
    )
    messages = swapped(messages, "feat")

    own, far, *near = call(
        sums_body, (shape((NODES, Q), F32), far_shape, *near_shape), flops=10**9
    )(messages, rowid)
    far = swapped(far, "graph")
    near = [moved(value, d) for value, d in zip(near, OFFSETS)]
    sums = call(spread_body, shape((FEAT, OWN, Q), BF16))(spread, own, far, *near)
    sums = swapped(sums, "feat")
    new_nodes = call(node_body, shape((OWN, D), BF16))(
        node_feats, sums, node_w1, node_w2, node_gain.reshape(1, D), node_shift.reshape(1, D)
    )
    return (new_edges, new_nodes)


def solution(mesh):
    split = P(("graph", "feat"))
    return jax.shard_map(
        per_device,
        mesh=mesh,
        in_specs=(split, split, split, split, P("graph"), P("graph")) + (P(),) * 8,
        out_specs=(split, split),
        check_vma=False,
    )
```

```python
import jax
import jax.numpy as jnp
from jax import lax
from jax.experimental import pallas as pl
from jax.experimental.pallas import tpu as pltpu
from jax.sharding import PartitionSpec as P

D = 512
Q = 128
FEAT = 4
GROUPS = 64
NODES = 320
OWN = 80
SLOT = 96
FAR = 16
NEAR = SLOT - FAR
EDGES = 512
REGION_EDGES = FEAT * EDGES
OFFSETS = (-2, -1, 1, 2)
FAR_ROWS = GROUPS * FAR
NEAR_ROWS = len(OFFSETS) * NEAR
LIST_ROWS = FAR_ROWS + NEAR_ROWS
TABLE_ROWS = NODES + LIST_ROWS
EPSILON = 1e-05
F32 = jnp.float32
BF16 = jnp.bfloat16
I32 = jnp.int32
VMEM = pl.BlockSpec(memory_space=pltpu.VMEM)
SMEM = pl.BlockSpec(memory_space=pltpu.SMEM)
HBM = pl.BlockSpec(memory_space=pltpu.HBM)


def dot(a, b):
    return jnp.dot(a, b, preferred_element_type=F32)


def iota(shape, dim):
    return lax.broadcasted_iota(I32, shape, dim)


def column(row):
    return jnp.transpose(jnp.broadcast_to(row, (Q, Q)))


def widened(tile, width):
    full, rest = divmod(width, Q)
    parts = [tile] * full + ([tile[:, :rest]] if rest else [])
    return jnp.concatenate(parts, axis=1)


def hot(mask):
    return jnp.where(mask, 1.0, 0.0).astype(BF16)


def call(body, outs, specs, scratch=(), flops=10**8, room=8):
    return pl.pallas_call(
        body,
        out_shape=outs,
        in_specs=specs,
        scratch_shapes=list(scratch),
        compiler_params=pltpu.CompilerParams(vmem_limit_bytes=room * 2**20),
        cost_estimate=pl.CostEstimate(flops=flops, bytes_accessed=10**6, transcendentals=0),
    )


def shape(dims, kind):
    return jax.ShapeDtypeStruct(dims, kind)


def peer(p):
    return (lax.axis_index("feat") + p) & (FEAT - 1)


def relative(node):
    owner = lax.shift_right_logical(node * 205, 14)
    return ((owner - lax.axis_index("feat")) & (FEAT - 1)) * OWN + node - owner * OWN


def project_body(nodes, w1, senders, refs, *rest):
    outs, (weights, ids, quarters, sems) = rest[:FEAT], rest[FEAT:]
    loads = [
        pltpu.make_async_copy(
            w1.at[pl.ds(D + k * D, D), :], weights.at[pl.ds(k * D, D), :], sems.at[k]
        )
        for k in range(2)
    ]
    for load in loads:
        load.start()
    rows = nodes[...]
    ids[0:4, :] = senders[...]
    ids[4:8, :] = refs[...]
    both = ids[...]
    planes = jnp.concatenate(
        [lax.shift_right_logical(both, 7).astype(F32), (both & 127).astype(F32)], axis=0
    ).astype(BF16)
    for k in range(2):
        loads[k].wait()
        product = dot(rows, weights[k * D : (k + 1) * D, :]).astype(BF16)
        for q in range(FEAT):
            quarters[q, :, (1 - k) * Q : (2 - k) * Q] = product[:, q * Q : (q + 1) * Q]
    for p, out in enumerate(outs):
        out[0:OWN, :] = quarters[peer(p)]
        out[OWN : OWN + 16, 0:Q] = planes
        out[OWN : OWN + 16, Q : 2 * Q] = jnp.zeros((16, Q), BF16)


def list_rows(lists, select):
    region = lax.axis_index("graph")
    across = iota((FAR, NODES), 1)
    flipped = jnp.transpose(
        jnp.concatenate([relative(lists[...]), jnp.zeros((GROUPS, Q - SLOT), I32)], axis=1)
    )
    for s in range(GROUPS):
        col = jnp.broadcast_to(flipped[0:FAR, s : s + 1], (FAR, NODES))
        select[s * FAR : (s + 1) * FAR, :] = hot(col == across)
    for j, d in enumerate(OFFSETS):
        row = relative(lists[pl.ds((region - d) & (GROUPS - 1), 1), :])
        row = jnp.concatenate([row, jnp.zeros((1, Q - SLOT), I32)], axis=1)
        col = column(row)[FAR:SLOT]
        at = FAR_ROWS + j * NEAR
        select[at : at + NEAR, :] = hot(widened(col, NODES) == iota((NEAR, NODES), 1))


def lists_body(lists, select):
    list_rows(lists, select)


def select_body(tile0, tile1, tile2, tile3, select, far, near0, near1, near2, near3):
    rows = jnp.concatenate(
        [tile[0:OWN, 0:Q] for tile in (tile0, tile1, tile2, tile3)], axis=0
    )
    for b in range(4):
        picked = dot(select[b * 256 : (b + 1) * 256, :], rows).astype(BF16)
        far[b * 16 : (b + 1) * 16] = picked.reshape(16, FAR, Q)
    for j, out in enumerate((near0, near1, near2, near3)):
        at = FAR_ROWS + j * NEAR
        out[...] = dot(select[at : at + NEAR, :], rows).astype(BF16)


def local_body(tile0, tile1, tile2, tile3, rowid, acc):
    region = lax.axis_index("graph")
    tiles = (tile0, tile1, tile2, tile3)
    both = jnp.concatenate(
        [tile[0:OWN, 0:Q] for tile in tiles] + [tile[0:OWN, Q : 2 * Q] for tile in tiles], axis=0
    )
    for p, tile in enumerate(tiles):
        planes = tile[OWN : OWN + 16, 0:Q].astype(F32)
        ids = (planes[0:8] * 128.0 + planes[8:16]).astype(I32)
        near = relative(ids)
        offset = jnp.maximum(ids - NODES, 0)
        source = lax.shift_right_logical(lax.shift_right_logical(offset, 5) * 171, 9)
        slot = offset - source * SLOT
        apart = (source - region) & (GROUPS - 1)
        which = jnp.where(apart >= GROUPS - 2, apart - (GROUPS - 2), apart + 1)
        listed = jnp.where(
            slot < FAR,
            NODES + source * FAR + slot,
            NODES + FAR_ROWS + which * NEAR + slot - FAR,
        )
        ref = jnp.where(ids < NODES, near, listed)
        rowid[p * 4 : (p + 1) * 4, :] = ref[4:8]
        for r in range(4):
            e = (p * 4 + r) * Q
            taken = column(ref[4 + r : 5 + r, :])
            sent = column(near[r : r + 1, :])
            picks = jnp.concatenate(
                [
                    hot(widened(taken, NODES) == iota((Q, NODES), 1)),
                    hot(widened(sent, NODES) == iota((Q, NODES), 1)),
                ],
                axis=1,
            )
            acc[e : e + Q, :] = dot(picks, both)


def gather_body(acc, rowid, far, near0, near1, near2, near3, *outs):
    table = [far[b * 16 : (b + 1) * 16].reshape(256, Q) for b in range(4)]
    table.append(jnp.concatenate([near0[...], near1[...], near2[...], near3[...]], axis=0))
    for p, out in enumerate(outs):
        for half in range(2):
            m = p * 2 + half
            col = jnp.concatenate(
                [column(rowid[2 * m + k : 2 * m + k + 1, :]) for k in range(2)], axis=0
            )
            total = acc[m * 256 : (m + 1) * 256, :]
            for b in range(5):
                width = table[b].shape[0]
                picks = hot(widened(col, width) == iota((256, width), 1) + (NODES + b * 256))
                total += dot(picks, table[b])
            out[half * 256 : (half + 1) * 256, :] = total.astype(BF16)


def wide(quarters):
    return jnp.concatenate([quarters[q : q + 1, :] for q in range(FEAT)], axis=1).astype(F32)


def normed(outputs, gain, shift):
    average = jnp.mean(outputs, axis=-1, keepdims=True)
    centered = outputs - average
    variance = jnp.mean(centered * centered, axis=-1, keepdims=True)
    return centered * lax.rsqrt(variance + EPSILON) * gain + shift


def silu(v):
    half = 0.5 * v
    return half + half * jnp.tanh(half)


def edge_body(count, edges, tile0, tile1, tile2, tile3, w1, w2, gain, shift, *rest):
    outs, (quarters, kept) = rest[:FEAT], rest[FEAT:]
    scale = wide(gain)
    move = wide(shift)
    first = lax.axis_index("feat") * EDGES
    for p, tile in enumerate((tile0, tile1, tile2, tile3)):
        quarters[peer(p)] = tile[...]
    for m in range(2):
        rows = slice(m * 256, (m + 1) * 256)
        feats = edges[rows, :]
        pre = dot(feats, w1[...])
        pre += jnp.concatenate([quarters[q, rows, :] for q in range(FEAT)], axis=1).astype(F32)
        hidden = silu(pre).astype(BF16)
        update = normed(dot(hidden, w2[...]), scale, move)
        live = first + m * 256 + iota((256, D), 0) < count[0]
        result = jnp.where(live, feats.astype(F32) + update, 0.0).astype(BF16)
        for q in range(FEAT):
            kept[q, rows, :] = result[:, q * Q : (q + 1) * Q]
    for p, out in enumerate(outs):
        out[...] = kept[peer(p)]


def finish_body(count, edges, tile0, tile1, tile2, tile3, out, done, kept):
    done[...] = jnp.zeros((8, Q), F32)
    first = lax.axis_index("feat") * EDGES
    for p, tile in enumerate((tile0, tile1, tile2, tile3)):
        kept[peer(p)] = tile[...]
    live = first + iota((EDGES, Q), 0) < count[0]
    for q in range(FEAT):
        cols = slice(q * Q, (q + 1) * Q)
        out[:, cols] = jnp.where(
            live, kept[q].astype(F32), edges[:, cols].astype(F32)
        ).astype(BF16)


BLOCKS = ((0, 320), (320, 256), (576, 256), (832, 256), (1088, 256), (1344, 320))


def block_sum(base, size, rowid, tile, p):
    total = jnp.zeros((size, Q), F32)
    for half in range(2):
        c = p * 4 + half * 2
        ids = jnp.concatenate([rowid[c : c + 1, :], rowid[c + 1 : c + 2, :]], axis=1)
        picks = hot(jnp.broadcast_to(ids, (size, 256)) == iota((size, 256), 0) + base)
        total += dot(picks, tile[half * 256 : (half + 1) * 256, :])
    return total


def first_sums_body(tile0, rowid, acc):
    for base, size in BLOCKS:
        acc[base : base + size, :] = block_sum(base, size, rowid, tile0, 0)


def sums_body(acc, tile1, tile2, tile3, rowid, own, far, near0, near1, near2, near3):
    for base, size in BLOCKS:
        total = acc[base : base + size, :]
        for p, tile in enumerate((tile1, tile2, tile3)):
            total += block_sum(base, size, rowid, tile, p + 1)
        if base == 0:
            own[...] = total
        elif base < NODES + FAR_ROWS:
            at = (base - NODES) // FAR
            far[at : at + 16] = total.astype(BF16).reshape(16, FAR, Q)
        else:
            for j, out in enumerate((near0, near1, near2, near3)):
                out[...] = total[j * NEAR : (j + 1) * NEAR].astype(BF16)


def flip_body(lists, spread, select):
    list_rows(lists, select)
    for at in range(0, LIST_ROWS, Q):
        size = min(Q, LIST_ROWS - at)
        spread[:, at : at + size] = jnp.transpose(select[at : at + size, :].astype(F32)).astype(
            BF16
        )


def spread_body(spread, own, far, near0, near1, near2, near3, after, *outs):
    total = own[...]
    for b in range(4):
        total += dot(
            spread[:, b * 256 : (b + 1) * 256], far[b * 16 : (b + 1) * 16].reshape(256, Q)
        )
    near = jnp.concatenate([near0[...], near1[...], near2[...], near3[...]], axis=0)
    total += dot(spread[:, FAR_ROWS:LIST_ROWS], near)
    total = total.astype(BF16)
    for p, out in enumerate(outs):
        out[...] = total[p * OWN : (p + 1) * OWN]


def node_body(nodes, tile0, tile1, tile2, tile3, w1, w2, gain, shift, out, quarters):
    feats = nodes[...]
    for p, tile in enumerate((tile0, tile1, tile2, tile3)):
        quarters[peer(p)] = tile[...]
    pre = dot(feats, w1[0:D, :])
    pre += dot(jnp.concatenate([quarters[q] for q in range(FEAT)], axis=1), w1[D : 2 * D, :])
    hidden = silu(pre).astype(BF16)
    update = normed(dot(hidden, w2[...]), wide(gain), wide(shift))
    out[...] = (feats.astype(F32) + update).astype(BF16)


def exchanged(tiles):
    arrived = [
        lax.ppermute(tiles[j], "feat", [(i, (i + j) % FEAT) for i in range(FEAT)])
        for j in (2, 1, 3)
    ]
    return tiles[0], arrived[2], arrived[0], arrived[1]


def swapped(value):
    return lax.all_to_all(value, "graph", split_axis=0, concat_axis=0, tiled=True)


def moved(value, by):
    return lax.ppermute(value, "graph", [(i, (i + by) % GROUPS) for i in range(GROUPS)])


def per_device(
    node_feats,
    edge_feats,
    senders,
    receiver_ref,
    send_list,
    edge_count,
    edge_w1,
    edge_w2,
    edge_gain,
    edge_shift,
    node_w1,
    node_w2,
    node_gain,
    node_shift,
):
    tiles = call(
        project_body,
        [shape((96, 256), BF16)] * FEAT,
        [VMEM, HBM, VMEM, VMEM],
        [
            pltpu.VMEM((2 * D, D), BF16),
            pltpu.VMEM((8, Q), I32),
            pltpu.VMEM((FEAT, OWN, 2 * Q), BF16),
            pltpu.SemaphoreType.DMA((2,)),
        ],
    )(node_feats, pltpu.with_memory_space_constraint(edge_w1, pltpu.HBM), senders.reshape(4, Q), receiver_ref.reshape(4, Q))
    tiles = exchanged(tiles)
    select = call(lists_body, shape((LIST_ROWS, NODES), BF16), [VMEM])(send_list[0])

    near_shape = [shape((NEAR, Q), BF16)] * 4
    far_shape = shape((GROUPS, FAR, Q), BF16)
    far, *near = call(select_body, (far_shape, *near_shape), [VMEM] * 5)(*tiles, select)
    far = swapped(far)
    near = [moved(value, -d) for value, d in zip(near, OFFSETS)]

    rowid, acc = call(
        local_body,
        (
            shape((16, Q), I32),
            shape((REGION_EDGES, Q), F32),
        ),
        [VMEM] * 4,
        flops=10**9,
    )(*tiles)
    quarter = [shape((EDGES, Q), BF16)] * FEAT
    picked = call(gather_body, quarter, [VMEM] * 7, flops=10**9)(acc, rowid, far, *near)
    picked = exchanged(picked)

    messages = call(
        edge_body,
        quarter,
        [SMEM] + [VMEM] * 9,
        [pltpu.VMEM((FEAT, EDGES, Q), BF16)] * 2,
        flops=10**9,
    )(
        edge_count,
        edge_feats,
        *picked,
        edge_w1[0:D],
        edge_w2,
        edge_gain.reshape(4, Q),
        edge_shift.reshape(4, Q),
    )
    arrived = exchanged(messages)
    partial = call(first_sums_body, shape((TABLE_ROWS, Q), F32), [VMEM] * 2, flops=10**8)(
        messages[0], rowid
    )
    own, far, *near = call(
        sums_body,
        (shape((NODES, Q), F32), far_shape, *near_shape),
        [VMEM] * 5,
        flops=10**9,
    )(partial, *arrived[1:], rowid)
    far = swapped(far)
    near = [moved(value, d) for value, d in zip(near, OFFSETS)]
    new_edges, done = call(
        finish_body,
        (shape((EDGES, D), BF16), shape((8, Q), F32)),
        [SMEM] + [VMEM] * 5,
        [pltpu.VMEM((FEAT, EDGES, Q), BF16)],
    )(edge_count, edge_feats, *messages)
    spread = call(
        flip_body,
        shape((NODES, LIST_ROWS), BF16),
        [VMEM],
        [pltpu.VMEM((LIST_ROWS, NODES), BF16)],
    )(send_list[0])
    sums = call(spread_body, [shape((OWN, Q), BF16)] * FEAT, [VMEM] * 8)(
        spread, own, far, *near, done
    )
    sums = exchanged(sums)
    new_nodes = call(
        node_body,
        shape((OWN, D), BF16),
        [VMEM] * 9,
        [pltpu.VMEM((FEAT, OWN, Q), BF16)],
    )(
        node_feats,
        *sums,
        node_w1,
        node_w2,
        node_gain.reshape(4, Q),
        node_shift.reshape(4, Q),
    )
    return (new_edges, new_nodes)


def solution(mesh):
    split = P(("graph", "feat"))
    return jax.shard_map(
        per_device,
        mesh=mesh,
        in_specs=(split, split, split, split, P("graph"), P("graph")) + (P(),) * 8,
        out_specs=(split, split),
        check_vma=False,
    )
```

```python
import functools

import jax
import jax.numpy as jnp
from jax import lax
from jax.experimental import pallas as pl
from jax.experimental.pallas import tpu as pltpu
from jax.sharding import PartitionSpec as P

D = 512
Q = 128
FEAT = 4
GROUPS = 64
NODES = 320
OWN = 80
SLOT = 96
FAR = 16
NEAR = SLOT - FAR
EDGES = 512
REGION_EDGES = FEAT * EDGES
OFFSETS = (-2, -1, 1, 2)
FAR_ROWS = GROUPS * FAR
NEAR_ROWS = len(OFFSETS) * NEAR
LIST_ROWS = FAR_ROWS + NEAR_ROWS
TABLE_ROWS = NODES + LIST_ROWS
EPSILON = 1e-05
F32 = jnp.float32
BF16 = jnp.bfloat16
I32 = jnp.int32
VMEM = pl.BlockSpec(memory_space=pltpu.VMEM)
SMEM = pl.BlockSpec(memory_space=pltpu.SMEM)
HBM = pl.BlockSpec(memory_space=pltpu.HBM)


def dot(a, b):
    return jnp.dot(a, b, preferred_element_type=F32)


def iota(shape, dim):
    return lax.broadcasted_iota(I32, shape, dim)


def column(row):
    return jnp.transpose(jnp.broadcast_to(row, (Q, Q)))


def widened(tile, width):
    full, rest = divmod(width, Q)
    parts = [tile] * full + ([tile[:, :rest]] if rest else [])
    return jnp.concatenate(parts, axis=1)


def hot(mask):
    return jnp.where(mask, 1.0, 0.0).astype(BF16)


def call(body, outs, specs, scratch=(), flops=10**8, room=8, alias=None):
    return pl.pallas_call(
        body,
        out_shape=outs,
        in_specs=specs,
        scratch_shapes=list(scratch),
        input_output_aliases=alias or {},
        compiler_params=pltpu.CompilerParams(vmem_limit_bytes=room * 2**20),
        cost_estimate=pl.CostEstimate(flops=flops, bytes_accessed=10**6, transcendentals=0),
    )


def shape(dims, kind):
    return jax.ShapeDtypeStruct(dims, kind)


def peer(p):
    return (lax.axis_index("feat") + p) & (FEAT - 1)


def relative(node):
    owner = lax.shift_right_logical(node * 205, 14)
    return ((owner - lax.axis_index("feat")) & (FEAT - 1)) * OWN + node - owner * OWN


def project_body(nodes_hbm, w1, senders, refs, *rest):
    outs, (nodes, weights, ids, quarters, sems) = rest[:FEAT], rest[FEAT:]
    loads = [
        pltpu.make_async_copy(nodes_hbm, nodes, sems.at[2]),
        pltpu.make_async_copy(w1.at[pl.ds(D, D), :], weights.at[pl.ds(0, D), :], sems.at[0]),
        pltpu.make_async_copy(w1.at[pl.ds(2 * D, D), :], weights.at[pl.ds(D, D), :], sems.at[1]),
        pltpu.make_async_copy(senders, ids.at[0], sems.at[3]),
        pltpu.make_async_copy(refs, ids.at[1], sems.at[4]),
    ]
    for load in loads:
        load.start()
    loads[3].wait()
    loads[4].wait()
    both = jnp.concatenate([ids[0], ids[1]], axis=0)
    planes = jnp.concatenate(
        [lax.shift_right_logical(both, 7).astype(F32), (both & 127).astype(F32)], axis=0
    ).astype(BF16)
    for out in outs:
        out[OWN : OWN + 16, 0:Q] = planes
        out[OWN : OWN + 16, Q : 2 * Q] = jnp.zeros((16, Q), BF16)
    loads[0].wait()
    rows = nodes[...]
    for k in range(2):
        loads[1 + k].wait()
        product = dot(rows, weights[k * D : (k + 1) * D, :]).astype(BF16)
        for q in range(FEAT):
            quarters[q, :, (1 - k) * Q : (2 - k) * Q] = product[:, q * Q : (q + 1) * Q]
    for p, out in enumerate(outs):
        out[0:OWN, :] = quarters[peer(p)]


def list_rows(lists, select):
    region = lax.axis_index("graph")
    across = iota((FAR, NODES), 1)
    flipped = jnp.transpose(
        jnp.concatenate([relative(lists[...]), jnp.zeros((GROUPS, Q - SLOT), I32)], axis=1)
    )
    for s in range(GROUPS):
        col = jnp.broadcast_to(flipped[0:FAR, s : s + 1], (FAR, NODES))
        select[s * FAR : (s + 1) * FAR, :] = hot(col == across)
    for j, d in enumerate(OFFSETS):
        row = relative(lists[pl.ds((region - d) & (GROUPS - 1), 1), :])
        row = jnp.concatenate([row, jnp.zeros((1, Q - SLOT), I32)], axis=1)
        col = column(row)[FAR:SLOT]
        at = FAR_ROWS + j * NEAR
        select[at : at + NEAR, :] = hot(widened(col, NODES) == iota((NEAR, NODES), 1))


def lists_body(lists, select):
    list_rows(lists, select)


def select_body(tile0, tile1, tile2, tile3, select, far, near0, near1, near2, near3):
    rows = jnp.concatenate(
        [tile[0:OWN, 0:Q] for tile in (tile0, tile1, tile2, tile3)], axis=0
    )
    for b in range(4):
        picked = dot(select[b * 256 : (b + 1) * 256, :], rows).astype(BF16)
        far[b * 16 : (b + 1) * 16] = picked.reshape(16, FAR, Q)
    for j, out in enumerate((near0, near1, near2, near3)):
        at = FAR_ROWS + j * NEAR
        out[...] = dot(select[at : at + NEAR, :], rows).astype(BF16)


def local_body(tile0, tile1, tile2, tile3, rowid, acc):
    region = lax.axis_index("graph")
    tiles = (tile0, tile1, tile2, tile3)
    both = jnp.concatenate(
        [tile[0:OWN, 0:Q] for tile in tiles] + [tile[0:OWN, Q : 2 * Q] for tile in tiles], axis=0
    )
    for p, tile in enumerate(tiles):
        planes = tile[OWN : OWN + 16, 0:Q].astype(F32)
        ids = (planes[0:8] * 128.0 + planes[8:16]).astype(I32)
        near = relative(ids)
        offset = jnp.maximum(ids - NODES, 0)
        source = lax.shift_right_logical(lax.shift_right_logical(offset, 5) * 171, 9)
        slot = offset - source * SLOT
        apart = (source - region) & (GROUPS - 1)
        which = jnp.where(apart >= GROUPS - 2, apart - (GROUPS - 2), apart + 1)
        listed = jnp.where(
            slot < FAR,
            NODES + source * FAR + slot,
            NODES + FAR_ROWS + which * NEAR + slot - FAR,
        )
        ref = jnp.where(ids < NODES, near, listed)
        rowid[p * 4 : (p + 1) * 4, :] = ref[4:8]
        for r in range(4):
            e = (p * 4 + r) * Q
            taken = column(ref[4 + r : 5 + r, :])
            sent = column(near[r : r + 1, :])
            picks = jnp.concatenate(
                [
                    hot(widened(taken, NODES) == iota((Q, NODES), 1)),
                    hot(widened(sent, NODES) == iota((Q, NODES), 1)),
                ],
                axis=1,
            )
            acc[e : e + Q, :] = dot(picks, both)


def gather_body(p, acc, rowid, far, near0, near1, near2, near3, out):
    table = [far[b * 16 : (b + 1) * 16].reshape(256, Q) for b in range(4)]
    table.append(jnp.concatenate([near0[...], near1[...], near2[...], near3[...]], axis=0))
    for half in range(2):
        m = p * 2 + half
        col = jnp.concatenate(
            [column(rowid[2 * m + k : 2 * m + k + 1, :]) for k in range(2)], axis=0
        )
        total = acc[m * 256 : (m + 1) * 256, :]
        for b in range(5):
            width = table[b].shape[0]
            picks = hot(widened(col, width) == iota((256, width), 1) + (NODES + b * 256))
            total += dot(picks, table[b])
        out[half * 256 : (half + 1) * 256, :] = total.astype(BF16)


def wide(quarters):
    return jnp.concatenate([quarters[q : q + 1, :] for q in range(FEAT)], axis=1).astype(F32)


def normed(outputs, gain, shift):
    average = jnp.mean(outputs, axis=-1, keepdims=True)
    centered = outputs - average
    variance = jnp.mean(centered * centered, axis=-1, keepdims=True)
    return centered * lax.rsqrt(variance + EPSILON) * gain + shift


def silu(v):
    half = 0.5 * v
    return half + half * jnp.tanh(half)


def edge_body(count, edges, tile0, tile1, tile2, tile3, w1, w2, gain, shift, *rest):
    outs, (quarters, kept) = rest[:FEAT], rest[FEAT:]
    scale = wide(gain)
    move = wide(shift)
    first = lax.axis_index("feat") * EDGES
    for p, tile in enumerate((tile0, tile1, tile2, tile3)):
        quarters[peer(p)] = tile[...]
    for m in range(2):
        rows = slice(m * 256, (m + 1) * 256)
        feats = edges[rows, :]
        pre = dot(feats, w1[...])
        pre += jnp.concatenate([quarters[q, rows, :] for q in range(FEAT)], axis=1).astype(F32)
        hidden = silu(pre).astype(BF16)
        update = normed(dot(hidden, w2[...]), scale, move)
        live = first + m * 256 + iota((256, D), 0) < count[0]
        result = jnp.where(live, feats.astype(F32) + update, 0.0).astype(BF16)
        for q in range(FEAT):
            kept[q, rows, :] = result[:, q * Q : (q + 1) * Q]
    for p, out in enumerate(outs):
        out[...] = kept[peer(p)]


def finish_body(count, edges, tile0, tile1, tile2, tile3, out, done, kept):
    done[...] = jnp.zeros((8, Q), F32)
    first = lax.axis_index("feat") * EDGES
    for p, tile in enumerate((tile0, tile1, tile2, tile3)):
        kept[peer(p)] = tile[...]
    live = first + iota((EDGES, Q), 0) < count[0]
    for q in range(FEAT):
        cols = slice(q * Q, (q + 1) * Q)
        out[:, cols] = jnp.where(
            live, kept[q].astype(F32), edges[:, cols].astype(F32)
        ).astype(BF16)


BLOCKS = ((0, 320), (320, 256), (576, 256), (832, 256), (1088, 256), (1344, 320))


def block_sum(base, size, rowid, tile, p):
    total = jnp.zeros((size, Q), F32)
    for half in range(2):
        c = p * 4 + half * 2
        ids = jnp.concatenate([rowid[c : c + 1, :], rowid[c + 1 : c + 2, :]], axis=1)
        picks = hot(jnp.broadcast_to(ids, (size, 256)) == iota((size, 256), 0) + base)
        total += dot(picks, tile[half * 256 : (half + 1) * 256, :])
    return total


def first_sums_body(tile, rowid, acc):
    for base, size in BLOCKS:
        acc[base : base + size, :] = block_sum(base, size, rowid, tile, 0)


def more_sums_body(p, acc, tile, rowid, out):
    for base, size in BLOCKS:
        rows = slice(base, base + size)
        out[rows, :] = acc[rows, :] + block_sum(base, size, rowid, tile, p)


def far_sums_body(acc, tile, rowid, done, far):
    for base, size in BLOCKS[1:5]:
        total = acc[base : base + size, :] + block_sum(base, size, rowid, tile, 2)
        at = (base - NODES) // FAR
        far[at : at + 16] = total.astype(BF16).reshape(16, FAR, Q)


def rest_sums_body(acc, tile, rowid, far, own, near0, near1, near2, near3):
    own[...] = acc[0:NODES, :] + block_sum(0, NODES, rowid, tile, 2)
    base = NODES + FAR_ROWS
    total = acc[base:TABLE_ROWS, :] + block_sum(base, NEAR_ROWS, rowid, tile, 2)
    for j, out in enumerate((near0, near1, near2, near3)):
        out[...] = total[j * NEAR : (j + 1) * NEAR].astype(BF16)


def flip_body(lists, spread, select):
    list_rows(lists, select)
    for at in range(0, LIST_ROWS, Q):
        size = min(Q, LIST_ROWS - at)
        spread[:, at : at + size] = jnp.transpose(select[at : at + size, :].astype(F32)).astype(
            BF16
        )


def spread_body(spread, own, far, near0, near1, near2, near3, *outs):
    total = own[...]
    for b in range(4):
        total += dot(
            spread[:, b * 256 : (b + 1) * 256], far[b * 16 : (b + 1) * 16].reshape(256, Q)
        )
    near = jnp.concatenate([near0[...], near1[...], near2[...], near3[...]], axis=0)
    total += dot(spread[:, FAR_ROWS:LIST_ROWS], near)
    total = total.astype(BF16)
    for p, out in enumerate(outs):
        out[...] = total[p * OWN : (p + 1) * OWN]


def node_body(nodes, tile0, tile1, tile2, tile3, w1, w2, gain, shift, out, quarters):
    feats = nodes[...]
    for p, tile in enumerate((tile0, tile1, tile2, tile3)):
        quarters[peer(p)] = tile[...]
    pre = dot(feats, w1[0:D, :])
    pre += dot(jnp.concatenate([quarters[q] for q in range(FEAT)], axis=1), w1[D : 2 * D, :])
    hidden = silu(pre).astype(BF16)
    update = normed(dot(hidden, w2[...]), wide(gain), wide(shift))
    out[...] = (feats.astype(F32) + update).astype(BF16)


def in_hbm(value):
    return pltpu.with_memory_space_constraint(value, pltpu.HBM)


def exchanged(tiles):
    arrived = [
        lax.ppermute(tiles[j], "feat", [(i, (i + j) % FEAT) for i in range(FEAT)])
        for j in (2, 1, 3)
    ]
    return tiles[0], arrived[2], arrived[0], arrived[1]


def swapped(value):
    return lax.all_to_all(value, "graph", split_axis=0, concat_axis=0, tiled=True)


def moved(value, by):
    return lax.ppermute(value, "graph", [(i, (i + by) % GROUPS) for i in range(GROUPS)])


def per_device(
    node_feats,
    edge_feats,
    senders,
    receiver_ref,
    send_list,
    edge_count,
    edge_w1,
    edge_w2,
    edge_gain,
    edge_shift,
    node_w1,
    node_w2,
    node_gain,
    node_shift,
):
    tiles = call(
        project_body,
        [shape((96, 256), BF16)] * FEAT,
        [HBM] * 4,
        [
            pltpu.VMEM((OWN, D), BF16),
            pltpu.VMEM((2 * D, D), BF16),
            pltpu.VMEM((2, 4, Q), I32),
            pltpu.VMEM((FEAT, OWN, 2 * Q), BF16),
            pltpu.SemaphoreType.DMA((5,)),
        ],
    )(*(in_hbm(x) for x in (node_feats, edge_w1, senders.reshape(4, Q), receiver_ref.reshape(4, Q))))
    tiles = exchanged(tiles)
    select = call(lists_body, shape((LIST_ROWS, NODES), BF16), [VMEM])(send_list[0])

    near_shape = [shape((NEAR, Q), BF16)] * 4
    far_shape = shape((GROUPS, FAR, Q), BF16)
    far, *near = call(select_body, (far_shape, *near_shape), [VMEM] * 5)(*tiles, select)
    far = swapped(far)
    near = [moved(value, -d) for value, d in zip(near, OFFSETS)]

    rowid, acc = call(
        local_body,
        (
            shape((16, Q), I32),
            shape((REGION_EDGES, Q), F32),
        ),
        [VMEM] * 4,
        flops=10**9,
    )(*tiles)
    quarter = [shape((EDGES, Q), BF16)] * FEAT
    picked = [
        call(functools.partial(gather_body, p), quarter[0], [VMEM] * 7)(acc, rowid, far, *near)
        for p in range(FEAT)
    ]
    picked = exchanged(picked)

    messages = call(
        edge_body,
        quarter,
        [SMEM] + [VMEM] * 9,
        [pltpu.VMEM((FEAT, EDGES, Q), BF16)] * 2,
        flops=10**9,
    )(
        edge_count,
        edge_feats,
        *picked,
        edge_w1[0:D],
        edge_w2,
        edge_gain.reshape(4, Q),
        edge_shift.reshape(4, Q),
    )
    new_edges, done = call(
        finish_body,
        (shape((EDGES, D), BF16), shape((8, Q), F32)),
        [SMEM] + [VMEM] * 5,
        [pltpu.VMEM((FEAT, EDGES, Q), BF16)],
    )(edge_count, edge_feats, *messages)
    arrived = exchanged(messages)
    acc_shape = shape((TABLE_ROWS, Q), F32)
    acc = call(first_sums_body, acc_shape, [VMEM] * 2)(messages[0], rowid)
    for p in (3, 1):
        acc = call(functools.partial(more_sums_body, p), acc_shape, [VMEM] * 3, alias={0: 0})(
            acc, arrived[p], rowid
        )
    sent = call(far_sums_body, far_shape, [VMEM] * 4)(acc, arrived[2], rowid, done)
    far = swapped(sent)
    own, *near = call(
        rest_sums_body, (shape((NODES, Q), F32), *near_shape), [VMEM] * 3 + [HBM]
    )(acc, arrived[2], rowid, sent)
    near = [moved(value, d) for value, d in zip(near, OFFSETS)]
    spread = call(
        flip_body,
        shape((NODES, LIST_ROWS), BF16),
        [VMEM],
        [pltpu.VMEM((LIST_ROWS, NODES), BF16)],
    )(send_list[0])
    sums = call(spread_body, [shape((OWN, Q), BF16)] * FEAT, [VMEM] * 7)(
        spread, own, far, *near
    )
    sums = exchanged(sums)
    new_nodes = call(
        node_body,
        shape((OWN, D), BF16),
        [VMEM] * 9,
        [pltpu.VMEM((FEAT, OWN, Q), BF16)],
    )(
        node_feats,
        *sums,
        node_w1,
        node_w2,
        node_gain.reshape(4, Q),
        node_shift.reshape(4, Q),
    )
    return (new_edges, new_nodes)


def solution(mesh):
    split = P(("graph", "feat"))
    return jax.shard_map(
        per_device,
        mesh=mesh,
        in_specs=(split, split, split, split, P("graph"), P("graph")) + (P(),) * 8,
        out_specs=(split, split),
        check_vma=False,
    )
```

```python
import functools

import jax
import jax.numpy as jnp
from jax import lax
from jax.experimental import pallas as pl
from jax.experimental.pallas import tpu as pltpu
from jax.sharding import PartitionSpec as P


D = 512
Q = 128
FEAT = 4
GROUPS = 64
NODES = 320
OWN = 80
SLOT = 96
FAR = 16
NEAR = SLOT - FAR
EDGES = 512
REGION_EDGES = FEAT * EDGES
OFFSETS = (-2, -1, 1, 2)
SEND_ORDER = (2, 1, 3)
FAR_ROWS = GROUPS * FAR
NEAR_ROWS = len(OFFSETS) * NEAR
LIST_ROWS = FAR_ROWS + NEAR_ROWS
TABLE_ROWS = NODES + LIST_ROWS
EPSILON = 1e-05
F32 = jnp.float32
BF16 = jnp.bfloat16
I32 = jnp.int32
VMEM = pl.BlockSpec(memory_space=pltpu.VMEM)
SMEM = pl.BlockSpec(memory_space=pltpu.SMEM)
HBM = pl.BlockSpec(memory_space=pltpu.HBM)


def dot(a, b):
    return jnp.dot(a, b, preferred_element_type=F32)


def iota(shape, dim):
    return lax.broadcasted_iota(I32, shape, dim)


def column(row):
    return jnp.transpose(jnp.broadcast_to(row, (Q, Q)))


def widened(tile, width):
    full, rest = divmod(width, Q)
    parts = [tile] * full + ([tile[:, :rest]] if rest else [])
    return jnp.concatenate(parts, axis=1)


def hot(mask):
    return jnp.where(mask, 1.0, 0.0).astype(BF16)


def call(body, outs, specs, scratch=(), flops=10**8, room=8, alias=None):
    return pl.pallas_call(
        body,
        out_shape=outs,
        in_specs=specs,
        scratch_shapes=list(scratch),
        input_output_aliases=alias or {},
        compiler_params=pltpu.CompilerParams(vmem_limit_bytes=room * 2**20),
        cost_estimate=pl.CostEstimate(flops=flops, bytes_accessed=10**6, transcendentals=0),
    )


def shape(dims, kind):
    return jax.ShapeDtypeStruct(dims, kind)


def peer(p):
    return lax.axis_index("feat") ^ p


def relative(node):
    owner = lax.shift_right_logical(node * 205, 14)
    return (owner ^ lax.axis_index("feat")) * OWN + node - owner * OWN


def project_body(nodes_hbm, w1, senders, refs, *rest):
    outs, (nodes, weights, ids, quarters, sems) = rest[:FEAT], rest[FEAT:]
    loads = [
        pltpu.make_async_copy(nodes_hbm, nodes, sems.at[2]),
        pltpu.make_async_copy(w1.at[pl.ds(D, D), :], weights.at[pl.ds(0, D), :], sems.at[0]),
        pltpu.make_async_copy(w1.at[pl.ds(2 * D, D), :], weights.at[pl.ds(D, D), :], sems.at[1]),
        pltpu.make_async_copy(senders, ids.at[0], sems.at[3]),
        pltpu.make_async_copy(refs, ids.at[1], sems.at[4]),
    ]
    for load in loads:
        load.start()
    loads[3].wait()
    loads[4].wait()
    both = jnp.concatenate([ids[0], ids[1]], axis=0)
    planes = jnp.concatenate(
        [lax.shift_right_logical(both, 7).astype(F32), (both & 127).astype(F32)], axis=0
    ).astype(BF16)
    for out in outs:
        out[OWN : OWN + 16, 0:Q] = planes
        out[OWN : OWN + 16, Q : 2 * Q] = jnp.zeros((16, Q), BF16)
    loads[0].wait()
    rows = nodes[...]
    for k in range(2):
        loads[1 + k].wait()
        product = dot(rows, weights[k * D : (k + 1) * D, :]).astype(BF16)
        for q in range(FEAT):
            quarters[q, :, (1 - k) * Q : (2 - k) * Q] = product[:, q * Q : (q + 1) * Q]
    for p, out in enumerate(outs):
        out[0:OWN, :] = quarters[peer(p)]


def list_rows(lists, select):
    region = lax.axis_index("graph")
    across = iota((FAR, NODES), 1)
    flipped = jnp.transpose(
        jnp.concatenate([relative(lists[...]), jnp.zeros((GROUPS, Q - SLOT), I32)], axis=1)
    )
    for s in range(GROUPS):
        col = jnp.broadcast_to(flipped[0:FAR, s : s + 1], (FAR, NODES))
        select[s * FAR : (s + 1) * FAR, :] = hot(col == across)
    for j, d in enumerate(OFFSETS):
        row = relative(lists[pl.ds((region - d) & (GROUPS - 1), 1), :])
        row = jnp.concatenate([row, jnp.zeros((1, Q - SLOT), I32)], axis=1)
        col = column(row)[FAR:SLOT]
        at = FAR_ROWS + j * NEAR
        select[at : at + NEAR, :] = hot(widened(col, NODES) == iota((NEAR, NODES), 1))


def lists_body(lists, select):
    list_rows(lists, select)


def select_body(tile0, tile1, tile2, tile3, select, far, near0, near1, near2, near3):
    rows = jnp.concatenate(
        [tile[0:OWN, 0:Q] for tile in (tile0, tile1, tile2, tile3)], axis=0
    )
    for b in range(4):
        picked = dot(select[b * 256 : (b + 1) * 256, :], rows).astype(BF16)
        far[b * 16 : (b + 1) * 16] = picked.reshape(16, FAR, Q)
    for j, out in enumerate((near0, near1, near2, near3)):
        at = FAR_ROWS + j * NEAR
        out[...] = dot(select[at : at + NEAR, :], rows).astype(BF16)


def local_body(tile0, tile1, tile2, tile3, rowid, acc):
    region = lax.axis_index("graph")
    tiles = (tile0, tile1, tile2, tile3)
    both = jnp.concatenate(
        [tile[0:OWN, 0:Q] for tile in tiles] + [tile[0:OWN, Q : 2 * Q] for tile in tiles], axis=0
    )
    for p, tile in enumerate(tiles):
        planes = tile[OWN : OWN + 16, 0:Q].astype(F32)
        ids = (planes[0:8] * 128.0 + planes[8:16]).astype(I32)
        near = relative(ids)
        offset = jnp.maximum(ids - NODES, 0)
        source = lax.shift_right_logical(lax.shift_right_logical(offset, 5) * 171, 9)
        slot = offset - source * SLOT
        apart = (source - region) & (GROUPS - 1)
        which = jnp.where(apart >= GROUPS - 2, apart - (GROUPS - 2), apart + 1)
        listed = jnp.where(
            slot < FAR,
            NODES + source * FAR + slot,
            NODES + FAR_ROWS + which * NEAR + slot - FAR,
        )
        ref = jnp.where(ids < NODES, near, listed)
        rowid[p * 4 : (p + 1) * 4, :] = ref[4:8]
        for r in range(4):
            e = (p * 4 + r) * Q
            taken = column(ref[4 + r : 5 + r, :])
            sent = column(near[r : r + 1, :])
            picks = jnp.concatenate(
                [
                    hot(widened(taken, NODES) == iota((Q, NODES), 1)),
                    hot(widened(sent, NODES) == iota((Q, NODES), 1)),
                ],
                axis=1,
            )
            acc[e : e + Q, :] = dot(picks, both)


def gather_body(p, acc, rowid, far, near0, near1, near2, near3, out):
    table = [far[b * 16 : (b + 1) * 16].reshape(256, Q) for b in range(4)]
    table.append(jnp.concatenate([near0[...], near1[...], near2[...], near3[...]], axis=0))
    for half in range(2):
        m = p * 2 + half
        col = jnp.concatenate(
            [column(rowid[2 * m + k : 2 * m + k + 1, :]) for k in range(2)], axis=0
        )
        total = acc[m * 256 : (m + 1) * 256, :]
        for b in range(5):
            width = table[b].shape[0]
            picks = hot(widened(col, width) == iota((256, width), 1) + (NODES + b * 256))
            total += dot(picks, table[b])
        out[half * 256 : (half + 1) * 256, :] = total.astype(BF16)


def wide(quarters):
    return jnp.concatenate([quarters[q : q + 1, :] for q in range(FEAT)], axis=1).astype(F32)


def normed(outputs, gain, shift):
    average = jnp.mean(outputs, axis=-1, keepdims=True)
    centered = outputs - average
    variance = jnp.mean(centered * centered, axis=-1, keepdims=True)
    return centered * lax.rsqrt(variance + EPSILON) * gain + shift


def silu(v):
    half = 0.5 * v
    return half + half * jnp.tanh(half)


def edge_body(count, edges, tile0, tile1, tile2, tile3, w1, w2, gain, shift, *rest):
    outs, (quarters, kept) = rest[:FEAT], rest[FEAT:]
    scale = wide(gain)
    move = wide(shift)
    first = lax.axis_index("feat") * EDGES
    for p, tile in enumerate((tile0, tile1, tile2, tile3)):
        quarters[peer(p)] = tile[...]
    for m in range(2):
        rows = slice(m * 256, (m + 1) * 256)
        feats = edges[rows, :]
        pre = dot(feats, w1[...])
        pre += jnp.concatenate([quarters[q, rows, :] for q in range(FEAT)], axis=1).astype(F32)
        hidden = silu(pre).astype(BF16)
        update = normed(dot(hidden, w2[...]), scale, move)
        live = first + m * 256 + iota((256, D), 0) < count[0]
        result = jnp.where(live, feats.astype(F32) + update, 0.0).astype(BF16)
        for q in range(FEAT):
            kept[q, rows, :] = result[:, q * Q : (q + 1) * Q]
    for p, out in enumerate(outs):
        out[...] = kept[peer(p)]


def finish_body(count, edges, tile0, tile1, tile2, tile3, out, done, kept):
    done[...] = jnp.zeros((8, Q), F32)
    first = lax.axis_index("feat") * EDGES
    for p, tile in enumerate((tile0, tile1, tile2, tile3)):
        kept[peer(p)] = tile[...]
    live = first + iota((EDGES, Q), 0) < count[0]
    for q in range(FEAT):
        cols = slice(q * Q, (q + 1) * Q)
        out[:, cols] = jnp.where(
            live, kept[q].astype(F32), edges[:, cols].astype(F32)
        ).astype(BF16)


BLOCKS = ((0, 320), (320, 256), (576, 256), (832, 256), (1088, 256), (1344, 320))


def block_sum(base, size, rowid, tile, p):
    total = jnp.zeros((size, Q), F32)
    for half in range(2):
        c = p * 4 + half * 2
        ids = jnp.concatenate([rowid[c : c + 1, :], rowid[c + 1 : c + 2, :]], axis=1)
        picks = hot(jnp.broadcast_to(ids, (size, 256)) == iota((size, 256), 0) + base)
        total += dot(picks, tile[half * 256 : (half + 1) * 256, :])
    return total


def first_sums_body(tile, rowid, acc):
    for base, size in BLOCKS:
        acc[base : base + size, :] = block_sum(base, size, rowid, tile, 0)


def more_sums_body(p, acc, tile, rowid, out):
    for base, size in BLOCKS:
        rows = slice(base, base + size)
        out[rows, :] = acc[rows, :] + block_sum(base, size, rowid, tile, p)


def far_sums_body(acc, tile, rowid, done, far):
    for base, size in BLOCKS[1:5]:
        total = acc[base : base + size, :] + block_sum(base, size, rowid, tile, SEND_ORDER[2])
        at = (base - NODES) // FAR
        far[at : at + 16] = total.astype(BF16).reshape(16, FAR, Q)


def rest_sums_body(acc, tile, rowid, far, own, near0, near1, near2, near3):
    own[...] = acc[0:NODES, :] + block_sum(0, NODES, rowid, tile, SEND_ORDER[2])
    base = NODES + FAR_ROWS
    total = acc[base:TABLE_ROWS, :] + block_sum(base, NEAR_ROWS, rowid, tile, SEND_ORDER[2])
    for j, out in enumerate((near0, near1, near2, near3)):
        out[...] = total[j * NEAR : (j + 1) * NEAR].astype(BF16)


def flip_body(lists, spread, select):
    list_rows(lists, select)
    for at in range(0, LIST_ROWS, Q):
        size = min(Q, LIST_ROWS - at)
        spread[:, at : at + size] = jnp.transpose(select[at : at + size, :].astype(F32)).astype(
            BF16
        )


def spread_body(spread, own, far, near0, near1, near2, near3, *outs):
    total = own[...]
    for b in range(4):
        total += dot(
            spread[:, b * 256 : (b + 1) * 256], far[b * 16 : (b + 1) * 16].reshape(256, Q)
        )
    near = jnp.concatenate([near0[...], near1[...], near2[...], near3[...]], axis=0)
    total += dot(spread[:, FAR_ROWS:LIST_ROWS], near)
    total = total.astype(BF16)
    for p, out in enumerate(outs):
        out[...] = total[p * OWN : (p + 1) * OWN]


def node_body(nodes, tile0, tile1, tile2, tile3, w1, w2, gain, shift, out, quarters):
    feats = nodes[...]
    for p, tile in enumerate((tile0, tile1, tile2, tile3)):
        quarters[peer(p)] = tile[...]
    pre = dot(feats, w1[0:D, :])
    pre += dot(jnp.concatenate([quarters[q] for q in range(FEAT)], axis=1), w1[D : 2 * D, :])
    hidden = silu(pre).astype(BF16)
    update = normed(dot(hidden, w2[...]), wide(gain), wide(shift))
    out[...] = (feats.astype(F32) + update).astype(BF16)


def in_hbm(value):
    return pltpu.with_memory_space_constraint(value, pltpu.HBM)


def exchanged(tiles):
    arrived = list(tiles)
    for p in SEND_ORDER:
        arrived[p] = lax.ppermute(tiles[p], "feat", [(i, i ^ p) for i in range(FEAT)])
    return arrived


def swapped(value):
    return lax.all_to_all(value, "graph", split_axis=0, concat_axis=0, tiled=True)


def moved(value, by):
    return lax.ppermute(value, "graph", [(i, (i + by) % GROUPS) for i in range(GROUPS)])


def per_device(
    node_feats,
    edge_feats,
    senders,
    receiver_ref,
    send_list,
    edge_count,
    edge_w1,
    edge_w2,
    edge_gain,
    edge_shift,
    node_w1,
    node_w2,
    node_gain,
    node_shift,
):
    tiles = call(
        project_body,
        [shape((96, 256), BF16)] * FEAT,
        [HBM] * 4,
        [
            pltpu.VMEM((OWN, D), BF16),
            pltpu.VMEM((2 * D, D), BF16),
            pltpu.VMEM((2, 4, Q), I32),
            pltpu.VMEM((FEAT, OWN, 2 * Q), BF16),
            pltpu.SemaphoreType.DMA((5,)),
        ],
    )(*(in_hbm(x) for x in (node_feats, edge_w1, senders.reshape(4, Q), receiver_ref.reshape(4, Q))))
    tiles = exchanged(tiles)
    select = call(lists_body, shape((LIST_ROWS, NODES), BF16), [VMEM])(send_list[0])

    near_shape = [shape((NEAR, Q), BF16)] * 4
    far_shape = shape((GROUPS, FAR, Q), BF16)
    far, *near = call(select_body, (far_shape, *near_shape), [VMEM] * 5)(*tiles, select)
    far = swapped(far)
    near = [moved(value, -d) for value, d in zip(near, OFFSETS)]

    rowid, acc = call(
        local_body,
        (
            shape((16, Q), I32),
            shape((REGION_EDGES, Q), F32),
        ),
        [VMEM] * 4,
        flops=10**9,
    )(*tiles)
    quarter = [shape((EDGES, Q), BF16)] * FEAT
    picked = [
        call(functools.partial(gather_body, p), quarter[0], [VMEM] * 7)(acc, rowid, far, *near)
        for p in range(FEAT)
    ]
    picked = exchanged(picked)

    messages = call(
        edge_body,
        quarter,
        [SMEM] + [VMEM] * 9,
        [pltpu.VMEM((FEAT, EDGES, Q), BF16)] * 2,
        flops=10**9,
    )(
        edge_count,
        edge_feats,
        *picked,
        edge_w1[0:D],
        edge_w2,
        edge_gain.reshape(4, Q),
        edge_shift.reshape(4, Q),
    )
    new_edges, done = call(
        finish_body,
        (shape((EDGES, D), BF16), shape((8, Q), F32)),
        [SMEM] + [VMEM] * 5,
        [pltpu.VMEM((FEAT, EDGES, Q), BF16)],
    )(edge_count, edge_feats, *messages)
    arrived = exchanged(messages)
    acc_shape = shape((TABLE_ROWS, Q), F32)
    acc = call(first_sums_body, acc_shape, [VMEM] * 2)(messages[0], rowid)
    for p in SEND_ORDER[:2]:
        acc = call(functools.partial(more_sums_body, p), acc_shape, [VMEM] * 3, alias={0: 0})(
            acc, arrived[p], rowid
        )
    sent = call(far_sums_body, far_shape, [VMEM] * 4)(acc, arrived[SEND_ORDER[2]], rowid, done)
    far = swapped(sent)
    own, *near = call(
        rest_sums_body, (shape((NODES, Q), F32), *near_shape), [VMEM] * 3 + [HBM]
    )(acc, arrived[SEND_ORDER[2]], rowid, sent)
    near = [moved(value, d) for value, d in zip(near, OFFSETS)]
    spread = call(
        flip_body,
        shape((NODES, LIST_ROWS), BF16),
        [VMEM],
        [pltpu.VMEM((LIST_ROWS, NODES), BF16)],
    )(send_list[0])
    sums = call(spread_body, [shape((OWN, Q), BF16)] * FEAT, [VMEM] * 7)(
        spread, own, far, *near
    )
    sums = exchanged(sums)
    new_nodes = call(
        node_body,
        shape((OWN, D), BF16),
        [VMEM] * 9,
        [pltpu.VMEM((FEAT, OWN, Q), BF16)],
    )(
        node_feats,
        *sums,
        node_w1,
        node_w2,
        node_gain.reshape(4, Q),
        node_shift.reshape(4, Q),
    )
    return (new_edges, new_nodes)


def solution(mesh):
    split = P(("graph", "feat"))
    return jax.shard_map(
        per_device,
        mesh=mesh,
        in_specs=(split, split, split, split, P("graph"), P("graph")) + (P(),) * 8,
        out_specs=(split, split),
        check_vma=False,
    )
```

```python
import functools

import jax
import jax.numpy as jnp
from jax import lax
from jax.experimental import pallas as pl
from jax.experimental.pallas import tpu as pltpu
from jax.sharding import PartitionSpec as P


D = 512
Q = 128
FEAT = 4
GROUPS = 64
NODES = 320
OWN = 80
SLOT = 96
FAR = 16
NEAR = SLOT - FAR
EDGES = 512
REGION_EDGES = FEAT * EDGES
OFFSETS = (-2, -1, 1, 2)
BLOCK = 512
ORDERS = {"table": (2, 3, 1), "picked": (2, 1, 3), "messages": (2, 1, 3), "sums": (2, 3, 1)}
SUM_ORDER = ORDERS["messages"]
FAR_ROWS = GROUPS * FAR
NEAR_ROWS = len(OFFSETS) * NEAR
LIST_ROWS = FAR_ROWS + NEAR_ROWS
TABLE_ROWS = NODES + LIST_ROWS
EPSILON = 1e-05
F32 = jnp.float32
BF16 = jnp.bfloat16
I32 = jnp.int32
VMEM = pl.BlockSpec(memory_space=pltpu.VMEM)
SMEM = pl.BlockSpec(memory_space=pltpu.SMEM)
HBM = pl.BlockSpec(memory_space=pltpu.HBM)


def dot(a, b):
    return jnp.dot(a, b, preferred_element_type=F32)


def iota(shape, dim):
    return lax.broadcasted_iota(I32, shape, dim)


def column(row):
    return jnp.transpose(jnp.broadcast_to(row, (Q, Q)))


def widened(tile, width):
    full, rest = divmod(width, Q)
    parts = [tile] * full + ([tile[:, :rest]] if rest else [])
    return jnp.concatenate(parts, axis=1)


def hot(mask):
    return jnp.where(mask, 1.0, 0.0).astype(BF16)


def call(body, outs, specs, scratch=(), flops=10**8, room=8, alias=None):
    return pl.pallas_call(
        body,
        out_shape=outs,
        in_specs=specs,
        scratch_shapes=list(scratch),
        input_output_aliases=alias or {},
        compiler_params=pltpu.CompilerParams(vmem_limit_bytes=room * 2**20),
        cost_estimate=pl.CostEstimate(flops=flops, bytes_accessed=10**6, transcendentals=0),
    )


def shape(dims, kind):
    return jax.ShapeDtypeStruct(dims, kind)


def peer(p):
    return lax.axis_index("feat") ^ p


def relative(node):
    owner = lax.shift_right_logical(node * 205, 14)
    return (owner ^ lax.axis_index("feat")) * OWN + node - owner * OWN


def project_body(nodes_hbm, w1, senders, refs, *rest):
    outs, (nodes, weights, ids, quarters, sems) = rest[:FEAT], rest[FEAT:]
    loads = [
        pltpu.make_async_copy(nodes_hbm, nodes, sems.at[2]),
        pltpu.make_async_copy(senders, ids.at[0], sems.at[3]),
        pltpu.make_async_copy(refs, ids.at[1], sems.at[4]),
        pltpu.make_async_copy(w1.at[pl.ds(D, D), :], weights.at[pl.ds(0, D), :], sems.at[0]),
        pltpu.make_async_copy(w1.at[pl.ds(2 * D, D), :], weights.at[pl.ds(D, D), :], sems.at[1]),
    ]
    for load in loads:
        load.start()
    loads[1].wait()
    loads[2].wait()
    both = jnp.concatenate([ids[0], ids[1]], axis=0)
    planes = jnp.concatenate(
        [lax.shift_right_logical(both, 7).astype(F32), (both & 127).astype(F32)], axis=0
    ).astype(BF16)
    for out in outs:
        out[OWN : OWN + 16, 0:Q] = planes
        out[OWN : OWN + 16, Q : 2 * Q] = jnp.zeros((16, Q), BF16)
    loads[0].wait()
    rows = nodes[...]
    for k in range(2):
        loads[3 + k].wait()
        product = dot(rows, weights[k * D : (k + 1) * D, :]).astype(BF16)
        for q in range(FEAT):
            quarters[q, :, (1 - k) * Q : (2 - k) * Q] = product[:, q * Q : (q + 1) * Q]
    for p, out in enumerate(outs):
        out[0:OWN, :] = quarters[peer(p)]


def list_rows(lists, select):
    region = lax.axis_index("graph")
    across = iota((FAR, NODES), 1)
    flipped = jnp.transpose(
        jnp.concatenate([relative(lists[...]), jnp.zeros((GROUPS, Q - SLOT), I32)], axis=1)
    )
    for s in range(GROUPS):
        col = jnp.broadcast_to(flipped[0:FAR, s : s + 1], (FAR, NODES))
        select[s * FAR : (s + 1) * FAR, :] = hot(col == across)
    for j, d in enumerate(OFFSETS):
        row = relative(lists[pl.ds((region - d) & (GROUPS - 1), 1), :])
        row = jnp.concatenate([row, jnp.zeros((1, Q - SLOT), I32)], axis=1)
        col = column(row)[FAR:SLOT]
        at = FAR_ROWS + j * NEAR
        select[at : at + NEAR, :] = hot(widened(col, NODES) == iota((NEAR, NODES), 1))


def lists_body(lists, select):
    list_rows(lists, select)


def select_body(tile0, tile1, tile2, tile3, select, far, near0, near1, near2, near3):
    rows = jnp.concatenate(
        [tile[0:OWN, 0:Q] for tile in (tile0, tile1, tile2, tile3)], axis=0
    )
    for b in range(4):
        picked = dot(select[b * 256 : (b + 1) * 256, :], rows).astype(BF16)
        far[b * 16 : (b + 1) * 16] = picked.reshape(16, FAR, Q)
    for j, out in enumerate((near0, near1, near2, near3)):
        at = FAR_ROWS + j * NEAR
        out[...] = dot(select[at : at + NEAR, :], rows).astype(BF16)


def local_body(tile0, tile1, tile2, tile3, rowid, acc):
    region = lax.axis_index("graph")
    tiles = (tile0, tile1, tile2, tile3)
    both = jnp.concatenate(
        [tile[0:OWN, 0:Q] for tile in tiles] + [tile[0:OWN, Q : 2 * Q] for tile in tiles], axis=0
    )
    for p, tile in enumerate(tiles):
        planes = tile[OWN : OWN + 16, 0:Q].astype(F32)
        ids = (planes[0:8] * 128.0 + planes[8:16]).astype(I32)
        near = relative(ids)
        offset = jnp.maximum(ids - NODES, 0)
        source = lax.shift_right_logical(lax.shift_right_logical(offset, 5) * 171, 9)
        slot = offset - source * SLOT
        apart = (source - region) & (GROUPS - 1)
        which = jnp.where(apart >= GROUPS - 2, apart - (GROUPS - 2), apart + 1)
        listed = jnp.where(
            slot < FAR,
            NODES + source * FAR + slot,
            NODES + FAR_ROWS + which * NEAR + slot - FAR,
        )
        ref = jnp.where(ids < NODES, near, listed)
        rowid[p * 4 : (p + 1) * 4, :] = ref[4:8]
        for r in range(4):
            e = (p * 4 + r) * Q
            taken = column(ref[4 + r : 5 + r, :])
            sent = column(near[r : r + 1, :])
            picks = jnp.concatenate(
                [
                    hot(widened(taken, NODES) == iota((Q, NODES), 1)),
                    hot(widened(sent, NODES) == iota((Q, NODES), 1)),
                ],
                axis=1,
            )
            acc[e : e + Q, :] = dot(picks, both)


def gather_body(p, acc, rowid, far, near0, near1, near2, near3, out):
    table = [far[b * 16 : (b + 1) * 16].reshape(256, Q) for b in range(4)]
    table.append(jnp.concatenate([near0[...], near1[...], near2[...], near3[...]], axis=0))
    for half in range(2):
        m = p * 2 + half
        col = jnp.concatenate(
            [column(rowid[2 * m + k : 2 * m + k + 1, :]) for k in range(2)], axis=0
        )
        total = acc[m * 256 : (m + 1) * 256, :]
        for b in range(5):
            width = table[b].shape[0]
            picks = hot(widened(col, width) == iota((256, width), 1) + (NODES + b * 256))
            total += dot(picks, table[b])
        out[half * 256 : (half + 1) * 256, :] = total.astype(BF16)


def wide(quarters):
    return jnp.concatenate([quarters[q : q + 1, :] for q in range(FEAT)], axis=1).astype(F32)


def normed(outputs, gain, shift):
    average = jnp.mean(outputs, axis=-1, keepdims=True)
    centered = outputs - average
    variance = jnp.mean(centered * centered, axis=-1, keepdims=True)
    return centered * lax.rsqrt(variance + EPSILON) * gain + shift


def silu(v):
    half = 0.5 * v
    return half + half * jnp.tanh(half)


def edge_body(count, edges, tile0, tile1, tile2, tile3, w1, w2, gain, shift, *rest):
    outs, (quarters, kept) = rest[:FEAT], rest[FEAT:]
    scale = wide(gain)
    move = wide(shift)
    first = lax.axis_index("feat") * EDGES
    for p, tile in enumerate((tile0, tile1, tile2, tile3)):
        quarters[peer(p)] = tile[...]
    for m in range(EDGES // BLOCK):
        rows = slice(m * BLOCK, (m + 1) * BLOCK)
        feats = edges[rows, :]
        pre = dot(feats, w1[...])
        pre += jnp.concatenate([quarters[q, rows, :] for q in range(FEAT)], axis=1).astype(F32)
        hidden = silu(pre).astype(BF16)
        update = normed(dot(hidden, w2[...]), scale, move)
        live = first + m * BLOCK + iota((BLOCK, D), 0) < count[0]
        result = jnp.where(live, feats.astype(F32) + update, 0.0).astype(BF16)
        for q in range(FEAT):
            kept[q, rows, :] = result[:, q * Q : (q + 1) * Q]
    for p, out in enumerate(outs):
        out[...] = kept[peer(p)]


def finish_body(count, edges, tile0, tile1, tile2, tile3, out, done, kept):
    done[...] = jnp.zeros((8, Q), F32)
    first = lax.axis_index("feat") * EDGES
    for p, tile in enumerate((tile0, tile1, tile2, tile3)):
        kept[peer(p)] = tile[...]
    live = first + iota((EDGES, Q), 0) < count[0]
    for q in range(FEAT):
        cols = slice(q * Q, (q + 1) * Q)
        out[:, cols] = jnp.where(
            live, kept[q].astype(F32), edges[:, cols].astype(F32)
        ).astype(BF16)


BLOCKS = ((0, 320), (320, 256), (576, 256), (832, 256), (1088, 256), (1344, 320))


def block_sum(base, size, rowid, tile, p):
    total = jnp.zeros((size, Q), F32)
    for half in range(2):
        c = p * 4 + half * 2
        ids = jnp.concatenate([rowid[c : c + 1, :], rowid[c + 1 : c + 2, :]], axis=1)
        picks = hot(jnp.broadcast_to(ids, (size, 256)) == iota((size, 256), 0) + base)
        total += dot(picks, tile[half * 256 : (half + 1) * 256, :])
    return total


def first_sums_body(tile, rowid, acc):
    for base, size in BLOCKS:
        acc[base : base + size, :] = block_sum(base, size, rowid, tile, 0)


def more_sums_body(p, acc, tile, rowid, out):
    for base, size in BLOCKS:
        rows = slice(base, base + size)
        out[rows, :] = acc[rows, :] + block_sum(base, size, rowid, tile, p)


def far_sums_body(acc, tile, rowid, done, far):
    for base, size in BLOCKS[1:5]:
        total = acc[base : base + size, :] + block_sum(base, size, rowid, tile, SUM_ORDER[2])
        at = (base - NODES) // FAR
        far[at : at + 16] = total.astype(BF16).reshape(16, FAR, Q)


def rest_sums_body(acc, tile, rowid, far, own, near0, near1, near2, near3):
    own[...] = acc[0:NODES, :] + block_sum(0, NODES, rowid, tile, SUM_ORDER[2])
    base = NODES + FAR_ROWS
    total = acc[base:TABLE_ROWS, :] + block_sum(base, NEAR_ROWS, rowid, tile, SUM_ORDER[2])
    for j, out in enumerate((near0, near1, near2, near3)):
        out[...] = total[j * NEAR : (j + 1) * NEAR].astype(BF16)


def flip_body(lists, spread, select):
    list_rows(lists, select)
    for at in range(0, LIST_ROWS, Q):
        size = min(Q, LIST_ROWS - at)
        spread[:, at : at + size] = jnp.transpose(select[at : at + size, :].astype(F32)).astype(
            BF16
        )


def spread_body(spread, own, far, near0, near1, near2, near3, *outs):
    total = own[...]
    for b in range(4):
        total += dot(
            spread[:, b * 256 : (b + 1) * 256], far[b * 16 : (b + 1) * 16].reshape(256, Q)
        )
    near = jnp.concatenate([near0[...], near1[...], near2[...], near3[...]], axis=0)
    total += dot(spread[:, FAR_ROWS:LIST_ROWS], near)
    total = total.astype(BF16)
    for p, out in enumerate(outs):
        out[...] = total[p * OWN : (p + 1) * OWN]


def begin_body(nodes, w1, after, out):
    out[...] = dot(nodes[...], w1[...])


def node_body(nodes, early, tile0, tile1, tile2, tile3, w1, w2, gain, shift, out, quarters):
    feats = nodes[...]
    for p, tile in enumerate((tile0, tile1, tile2, tile3)):
        quarters[peer(p)] = tile[...]
    pre = early[...]
    pre += dot(jnp.concatenate([quarters[q] for q in range(FEAT)], axis=1), w1[...])
    hidden = silu(pre).astype(BF16)
    update = normed(dot(hidden, w2[...]), wide(gain), wide(shift))
    out[...] = (feats.astype(F32) + update).astype(BF16)


def in_hbm(value):
    return pltpu.with_memory_space_constraint(value, pltpu.HBM)


def exchanged(tiles, name):
    arrived = list(tiles)
    for p in ORDERS[name]:
        arrived[p] = lax.ppermute(tiles[p], "feat", [(i, i ^ p) for i in range(FEAT)])
    return arrived


def swapped(value):
    return lax.all_to_all(value, "graph", split_axis=0, concat_axis=0, tiled=True)


def moved(value, by):
    return lax.ppermute(value, "graph", [(i, (i + by) % GROUPS) for i in range(GROUPS)])


def per_device(
    node_feats,
    edge_feats,
    senders,
    receiver_ref,
    send_list,
    edge_count,
    edge_w1,
    edge_w2,
    edge_gain,
    edge_shift,
    node_w1,
    node_w2,
    node_gain,
    node_shift,
):
    tiles = call(
        project_body,
        [shape((96, 256), BF16)] * FEAT,
        [HBM] * 4,
        [
            pltpu.VMEM((OWN, D), BF16),
            pltpu.VMEM((2 * D, D), BF16),
            pltpu.VMEM((2, 4, Q), I32),
            pltpu.VMEM((FEAT, OWN, 2 * Q), BF16),
            pltpu.SemaphoreType.DMA((5,)),
        ],
    )(*(in_hbm(x) for x in (node_feats, edge_w1, senders.reshape(4, Q), receiver_ref.reshape(4, Q))))
    tiles = exchanged(tiles, "table")
    select = call(lists_body, shape((LIST_ROWS, NODES), BF16), [VMEM])(send_list[0])

    near_shape = [shape((NEAR, Q), BF16)] * 4
    far_shape = shape((GROUPS, FAR, Q), BF16)
    far, *near = call(select_body, (far_shape, *near_shape), [VMEM] * 5)(*tiles, select)
    far = swapped(far)
    near = [moved(value, -d) for value, d in zip(near, OFFSETS)]

    rowid, acc = call(
        local_body,
        (
            shape((16, Q), I32),
            shape((REGION_EDGES, Q), F32),
        ),
        [VMEM] * 4,
        flops=10**9,
    )(*tiles)
    quarter = [shape((EDGES, Q), BF16)] * FEAT
    picked = [
        call(functools.partial(gather_body, p), quarter[0], [VMEM] * 7)(acc, rowid, far, *near)
        for p in range(FEAT)
    ]
    picked = exchanged(picked, "picked")

    messages = call(
        edge_body,
        quarter,
        [SMEM] + [VMEM] * 9,
        [pltpu.VMEM((FEAT, EDGES, Q), BF16)] * 2,
        flops=10**9,
    )(
        edge_count,
        edge_feats,
        *picked,
        edge_w1[0:D],
        edge_w2,
        edge_gain.reshape(4, Q),
        edge_shift.reshape(4, Q),
    )
    new_edges, done = call(
        finish_body,
        (shape((EDGES, D), BF16), shape((8, Q), F32)),
        [SMEM] + [VMEM] * 5,
        [pltpu.VMEM((FEAT, EDGES, Q), BF16)],
    )(edge_count, edge_feats, *messages)
    arrived = exchanged(messages, "messages")
    acc_shape = shape((TABLE_ROWS, Q), F32)
    acc = call(first_sums_body, acc_shape, [VMEM] * 2)(messages[0], rowid)
    for p in SUM_ORDER[:2]:
        acc = call(functools.partial(more_sums_body, p), acc_shape, [VMEM] * 3, alias={0: 0})(
            acc, arrived[p], rowid
        )
    sent = call(far_sums_body, far_shape, [VMEM] * 4)(acc, arrived[SUM_ORDER[2]], rowid, done)
    far = swapped(sent)
    own, *near = call(
        rest_sums_body, (shape((NODES, Q), F32), *near_shape), [VMEM] * 3 + [HBM]
    )(acc, arrived[SUM_ORDER[2]], rowid, sent)
    near = [moved(value, d) for value, d in zip(near, OFFSETS)]
    spread = call(
        flip_body,
        shape((NODES, LIST_ROWS), BF16),
        [VMEM],
        [pltpu.VMEM((LIST_ROWS, NODES), BF16)],
    )(send_list[0])
    early = call(begin_body, shape((OWN, D), F32), [VMEM] * 3)(node_feats, node_w1[0:D], own)
    sums = call(spread_body, [shape((OWN, Q), BF16)] * FEAT, [VMEM] * 7)(
        spread, own, far, *near
    )
    sums = exchanged(sums, "sums")
    new_nodes = call(
        node_body,
        shape((OWN, D), BF16),
        [VMEM] * 10,
        [pltpu.VMEM((FEAT, OWN, Q), BF16)],
    )(
        node_feats,
        early,
        *sums,
        node_w1[D : 2 * D],
        node_w2,
        node_gain.reshape(4, Q),
        node_shift.reshape(4, Q),
    )
    return (new_edges, new_nodes)


def solution(mesh):
    split = P(("graph", "feat"))
    return jax.shard_map(
        per_device,
        mesh=mesh,
        in_specs=(split, split, split, split, P("graph"), P("graph")) + (P(),) * 8,
        out_specs=(split, split),
        check_vma=False,
    )
```
